128 devices in a mesh: row: 8 (over y, core), col: 16 (over z, x).
Axes of the slice: x: 4, y: 4, z: 4, core: 2. Of those that a mesh axis runs over, the one named last changes fastest.
Arguments:
- text_features: bfloat16 [5, 4096, 3584], P(None, ('row', 'col')), may hold values from -18 to 18
- vision_features: bfloat16 [6, 4096, 1024], P(None, ('row', 'col')), may hold values from -18 to 18
Outputs:
- stimulus_terms: float32 [4096, 30], P(('row', 'col'))
- cka: float32 [5, 6], replicated
The draws below stay inside these ranges and needn't reach their ends.
All inputs are finite; a program needn't handle non-finite values.
Results may differ from the reference program's by a relative error of at most 0.0003.
Values may be sent and summed in bfloat16 or wider, within the bound.
A program may use at most 192 MiB of HBM per device.

```python
import math
import jax
import jax.numpy as jnp
from jax import lax

DA = 3584
DB = 1024
LA = 5
LB = 6
STIMULI = 4096


def shared_latent(key):
    key_latent = jax.random.fold_in(key, 21)
    key_scale = jax.random.fold_in(key, 22)
    latent = jax.random.truncated_normal(key_latent, -4.0, 4.0, (STIMULI, DB // 4), jnp.float32)
    top_scale = math.log(3.0)
    scales = jnp.exp(jax.random.uniform(key_scale, (STIMULI, 1), jnp.float32, 0.0, top_scale))
    return latent * scales


def feature_draw(key, modality, layers, width):
    latent = shared_latent(key)
    own_key = jax.random.fold_in(key, modality)
    key_offset = jax.random.fold_in(own_key, 11)
    key_noise = jax.random.fold_in(own_key, 12)
    key_project = jax.random.fold_in(own_key, 13)
    key_strength = jax.random.fold_in(own_key, 14)
    offsets = jax.random.uniform(key_offset, (layers, 1, width), jnp.float32, -2.0, 2.0)
    noise = jax.random.truncated_normal(key_noise, -4.0, 4.0, (layers, STIMULI, width), jnp.float32)
    projection = jax.random.truncated_normal(key_project, -4.0, 4.0, (layers, DB // 4, width), jnp.float32) * (DB // 4) ** (-0.5)
    strength = jax.random.uniform(key_strength, (layers, 1, 1), jnp.float32, 0.5, 0.9)
    signal = jnp.einsum('sr,lrw->lsw', latent, projection, precision=lax.Precision.HIGHEST) * strength
    values = jnp.clip(noise + signal, -16.0, 16.0) + offsets
    return values.astype(jnp.bfloat16)


def draw_text_features(key, part):
    return feature_draw(key, 1, LA, DA)


def draw_vision_features(key, part):
    return feature_draw(key, 2, LB, DB)


def setup_inputs(seed: int = 0) -> dict:
    arg_keys = jax.random.split(jax.random.key(seed), 3)
    return {
        "text_features": draw_text_features(jax.random.fold_in(arg_keys[2], 71), 0),
        "vision_features": draw_vision_features(jax.random.fold_in(arg_keys[2], 71), 0),
    }


def center_features(features):
    values = features.astype(jnp.float32)
    mean_values = lax.optimization_barrier(jnp.sum(values, axis=1, keepdims=True)) / values.shape[1]
    return (values - mean_values).astype(jnp.bfloat16)

def reference(text_features, vision_features):
    text_centered = center_features(text_features)
    vision_centered = center_features(vision_features).astype(jnp.float32)
    vision_grams = jnp.einsum('lsd,ltd->lst', vision_centered, vision_centered, precision=lax.Precision.HIGHEST)
    vision_self = lax.optimization_barrier(jnp.sum(vision_grams * vision_grams, axis=(1, 2)))

    def per_text(layer_feats):
        gram = jnp.dot(layer_feats, layer_feats.T, preferred_element_type=jnp.float32)
        share = jnp.einsum('st,mst->sm', gram, vision_grams, precision=lax.Precision.HIGHEST)
        return (share, jnp.sum(gram * gram))
    row_share, text_self = lax.map(per_text, text_centered)
    scale = 1.0 / jnp.sqrt(text_self[:, None] * vision_self[None, :])
    cross = lax.optimization_barrier(jnp.sum(row_share, axis=1))
    cka = cross * scale
    terms = jnp.transpose(row_share, (1, 0, 2)) * scale[None] * STIMULI
    return (terms.reshape(STIMULI, LA * LB), cka)
```

```python
import jax
import jax.numpy as jnp
from jax import lax
from jax.experimental import pallas as pl
from jax.experimental.pallas import tpu as pltpu
from jax.sharding import Mesh
from jax.sharding import PartitionSpec as P

STIMULI = 4096
LA, LB = 5, 6
BLOCKS = (
    (0, 1, 0), (0, 0, 2), (3, 0, 0), (2, 0, 0), (1, 3, 0), (1, 1, 1),
    (0, 1, 1), (0, 1, 2), (0, 0, 0), (2, 3, 0), (0, 0, 3), (0, 3, 0),
)
OWN = 8
STRIPS = ((2, 4, 5, 10, 11), (1, 5, 10, 11), (0, 1, 3, 7, 8, 10, 11), (1, 3, 4, 9, 11), (0, 1, 5, 6, 10), (3, 4, 5, 6, 9, 10))
STEPS = ((1, 0, 0), (3, 0, 0), (0, 1, 0), (0, 3, 0), (0, 0, 1), (0, 0, 3))
EDGES = (
    ((8, 0, 2), (8, 2, 1), (8, 10, 5), (8, 11, 3)),
    ((10, 1, 5), (2, 3, 1), (11, 4, 0), (0, 6, 4)),
    ((6, 5, 0), (1, 7, 2), (3, 9, 3)),
)
CHUNKS, WIDTH = 24, 512
ROWS, HALF = 64, 32
ALL = len(BLOCKS) * ROWS
AHEAD, LAG, LATE = 3, 2, 2
LAST = (3, 10, 17, 19, 21, 23)
F32, BF16 = jnp.float32, jnp.bfloat16
MESH = pl.DeviceIdType.MESH


def kernel(
    text, vision, terms, cka,
    buf, acc, rx, xc, sums, mrx, rs, selfs, rrx, row, ar1, ar2,
    load_sem, swap_send, swap_recv, mean_send, mean_recv, hop_send, hop_recv,
    ex_send, ex_recv, rs_send, rs_recv, ar1_send, ar1_recv, ar2_send, ar2_recv,
):
    y, p = lax.axis_index("row_0"), lax.axis_index("row_1")
    z, x = lax.axis_index("col_0"), lax.axis_index("col_1")

    def at(offset, core):
        dx, dy, dz = offset
        return (lax.rem(y + dy, 4), core, lax.rem(z + dz, 4), lax.rem(x + dx, 4))

    def back(step):
        return tuple((4 - v) % 4 for v in step)

    def remote(src, dst, send, recv, device):
        return pltpu.make_async_remote_copy(
            src_ref=src, dst_ref=dst, send_sem=send, recv_sem=recv, device_id=device, device_id_type=MESH
        )

    other = 1 - p
    here = (0, 0, 0)

    def source(c, core):
        if c < 4:
            return text.at[2, :, pl.ds(pl.multiple_of(core * 1536 + c * WIDTH, WIDTH), WIDTH)]
        if c < 11:
            return text.at[core * 3, :, pl.ds((c - 4) * WIDTH, WIDTH)]
        if c < 18:
            return text.at[core * 3 + 1, :, pl.ds((c - 11) * WIDTH, WIDTH)]
        return vision.at[core * 3 + (c - 18) // 2, :, pl.ds((c - 18) % 2 * WIDTH, WIDTH)]

    mine = pl.ds(pl.multiple_of(OWN * ROWS + p * HALF, HALF), HALF)

    def load(c):
        return pltpu.make_async_copy(source(c, p), buf.at[c, mine, :], load_sem.at[c])

    def swap(c):
        return remote(source(c, other), buf.at[c, mine, :], swap_send.at[c], swap_recv.at[c], at(here, other))

    for c in range(CHUNKS):
        if c == 0:
            pl.when(p == 0)(lambda: load(0).start())
            pl.when(p == 1)(lambda: swap(0).start())
        else:
            load(c).start()
            swap(c).start()

    @pl.loop(0, 36)
    def _(i):
        acc[i // 6, i % 6] = jnp.zeros((ALL, 128), F32)

    rs[...] = jnp.zeros_like(rs)
    selfs[...] = jnp.zeros_like(selfs)

    sums[0, 0:1, :] = jnp.zeros((1, WIDTH), F32)
    ones = jnp.ones((8, ROWS), BF16)

    @pl.loop(p, CHUNKS)
    def _(c):
        part = buf.at[c, mine, :]
        pltpu.make_async_copy(part, part, load_sem.at[c]).wait()
        pltpu.make_async_copy(part, part, swap_recv.at[c]).wait()
        total = jnp.dot(ones, buf[c, OWN * ROWS : (OWN + 1) * ROWS, :], preferred_element_type=F32)
        sums[0, pl.ds(c, 1), :] = total[0:1]

    def hop(edge, c):
        held, becomes, step = edge
        return remote(
            buf.at[c, pl.ds(held * ROWS, ROWS), :],
            buf.at[c, pl.ds(becomes * ROWS, ROWS), :],
            hop_send.at[c],
            hop_recv.at[c, becomes],
            at(back(STEPS[step]), p),
        )

    def arrived(block, c):
        part = buf.at[c, pl.ds(block * ROWS, ROWS), :]
        pltpu.make_async_copy(part, part, hop_recv.at[c, block]).wait()

    def send_own(c):
        for edge in EDGES[0]:
            hop(edge, c).start()

    def mean_copy(axis, k):
        offset = tuple(k if i == axis else 0 for i in range(3))
        return remote(
            sums.at[axis], mrx.at[axis, k - 1], mean_send.at[axis, k - 1], mean_recv.at[axis, k - 1], at(offset, p)
        )

    for axis in range(3):
        for k in (1, 2, 3):
            mean_copy(axis, k).start()
        if axis == 0:
            pl.when(p == 0)(lambda: send_own(0))
        else:
            send_own(axis)
        for k in (1, 2, 3):
            mean_copy(axis, k).wait_recv()
        sums[axis + 1] = (sums[axis] + mrx[axis, 0]) + (mrx[axis, 1] + mrx[axis, 2])

    inner = [sorted({e[0] for e in EDGES[d]}) for d in range(3)]
    leaves = [e[1] for d in EDGES for e in d if all(e[1] not in s for s in inner)]

    def exchange(layer):
        return remote(
            acc.at[layer, pl.ds(other * 3, 3)], rx.at[layer], ex_send.at[layer], ex_recv.at[layer], at(here, other)
        )

    def compute(c):
        for block in leaves:
            arrived(block, c)
        mean = sums[3, pl.ds(c, 1), :] * (1.0 / STIMULI)
        xc[...] = (buf[c].astype(F32) - mean).astype(BF16)
        layer = jnp.where(c < 4, 0, jnp.where(c < 11, 1, jnp.where(c < 18, 2, 3 + (c - 18) // 2)))
        for g in range(3):
            tile = lax.dot_general(
                xc[...],
                xc[g * 256 : (g + 1) * 256, :],
                (((1,), (1,)), ((), ())),
                preferred_element_type=F32,
            )
            acc[layer, 2 * g] += tile[:, :128]
            acc[layer, 2 * g + 1] += tile[:, 128:]
        for layer, last in enumerate(LAST):
            pl.when(c == last)(lambda layer=layer: exchange(layer).start())

    @pl.loop(min(AHEAD, LAG), CHUNKS + 2 * LAG + LATE)
    def _(u):
        @pl.when((u >= AHEAD) & (u < CHUNKS))
        def _():
            send_own(u)

        for depth in (1, 2):
            c = u - depth * LAG

            @pl.when((c >= p) & (c < CHUNKS))
            def _():
                for block in inner[depth]:
                    arrived(block, c)
                for edge in EDGES[depth]:
                    hop(edge, c).start()

        c = u - 2 * LAG - LATE

        @pl.when((c >= p) & (c < CHUNKS))
        def _():
            compute(c)

    for layer in range(6):
        exchange(layer).wait_recv()

    def products(core):
        texts = (0, 1, 2, 3, 4) if core == 0 else (3, 4, 2, 0, 1)
        for i in range(3):
            q = core * 3 + i
            for k in range(3):
                n_text = LA if k == 0 else 0

                def body(r, sums_):
                    s = list(sums_)
                    for block in STRIPS[q]:
                        at_ = pl.ds(pl.multiple_of(block * ROWS + r * 8, 8), 8)
                        t = (
                            acc[1, q, at_, :],
                            acc[2, q, at_, :],
                            acc[0, q, at_, :] + rx[0, i, at_, :],
                            rx[1, i, at_, :],
                            rx[2, i, at_, :],
                        )
                        v = (acc[3 + k, q, at_, :], rx[3 + k, i, at_, :])
                        for a in range(LA):
                            for b in range(2):
                                s[2 * a + b] += t[a] * v[b]
                        for b in range(2):
                            s[10 + b] += v[b] * v[b]
                        for a in range(n_text):
                            s[12 + a] += t[a] * t[a]
                    return tuple(s)

                zero = jnp.zeros((8, 128), F32)
                s = lax.fori_loop(0, 8, body, (zero,) * (12 + n_text))
                visions = (core * 3 + k, (1 - core) * 3 + k)
                for a in range(LA):
                    for b in range(2):
                        n = texts[a] * LB + visions[b]
                        rs[i, n : n + 1, :] = jnp.sum(s[2 * a + b], axis=0, keepdims=True)
                for b in range(2):
                    n = 8 + visions[b]
                    selfs[n : n + 1, :] += jnp.sum(s[10 + b], axis=0, keepdims=True)
                for a in range(n_text):
                    n = texts[a]
                    selfs[n : n + 1, :] += jnp.sum(s[12 + a], axis=0, keepdims=True)

            for j in (2 * q, 2 * q + 1):
                for to in (0, 1):
                    if j == OWN and to == core:
                        rrx[j] = rs[i]
                    else:
                        share(i, j, to).start()

    def share(i, j, to):
        return remote(rs.at[i], rrx.at[j], rs_send.at[i, j % 2, to], rs_recv.at[j], at(BLOCKS[j], to))

    for core in (0, 1):
        pl.when(p == core)(lambda core=core: products(core))

    cross = rs[0] + rs[1] + rs[2]
    parts = jnp.concatenate([cross, selfs[...]], axis=0)
    parts = jnp.sum(parts, axis=1, keepdims=True)
    lane = lax.broadcasted_iota(jnp.int32, (48, 128), 1)
    sub = lax.broadcasted_iota(jnp.int32, (48, 128), 0)
    row[0] = jnp.sum(jnp.where(lane == sub, parts, 0.0), axis=0, keepdims=True)

    plane = [(dx, dy) for dx in range(4) for dy in range(4) if dx or dy]
    me1 = x * 4 + y

    def over_plane(n):
        dx, dy = plane[n]
        return remote(row.at[0], ar1.at[me1], ar1_send.at[n], ar1_recv.at[me1], at((dx, dy, 0), p))

    for n in range(15):
        over_plane(n).start()
    ar1[me1] = row[0]
    for dx, dy in plane:
        n = lax.rem(x + dx, 4) * 4 + lax.rem(y + dy, 4)
        pltpu.make_async_copy(ar1.at[n], ar1.at[n], ar1_recv.at[n]).wait()
    row[1] = jnp.sum(ar1[...], axis=0)

    column = [(dz, dc) for dz in range(4) for dc in range(2) if dz or dc]
    me2 = z * 2 + p

    def over_column(n):
        dz, dc = column[n]
        return remote(
            row.at[1], ar2.at[me2], ar2_send.at[n], ar2_recv.at[me2], at((0, 0, dz), other if dc else p)
        )

    for n in range(7):
        over_column(n).start()
    ar2[me2] = row[1]
    for dz, dc in column:
        n = lax.rem(z + dz, 4) * 2 + (other if dc else p)
        pltpu.make_async_copy(ar2.at[n], ar2.at[n], ar2_recv.at[n]).wait()
    total = jnp.sum(ar2[...], axis=0)

    def pick(index, n):
        lanes = lax.broadcasted_iota(jnp.int32, (n, 128), 1)
        return jnp.sum(jnp.where(lanes == index, total, 0.0), axis=1, keepdims=True)

    pair = lax.broadcasted_iota(jnp.int32, (32, 1), 0)
    of_text, of_vision = pair // LB, lax.rem(pair, LB)
    scale = 1.0 / jnp.sqrt(pick(32 + jnp.minimum(of_text, LA - 1), 32) * pick(40 + of_vision, 32))
    for j in range(len(BLOCKS)):
        if j == OWN:
            pl.when(p != OWN // 6)(lambda: pltpu.make_async_copy(rrx.at[OWN], rrx.at[OWN], rs_recv.at[OWN]).wait())
        else:
            pltpu.make_async_copy(rrx.at[j], rrx.at[j], rs_recv.at[j]).wait()
    even = ((rrx[0] + rrx[2]) + (rrx[4] + rrx[6])) + (rrx[8] + rrx[10])
    odd = ((rrx[1] + rrx[3]) + (rrx[5] + rrx[7])) + (rrx[9] + rrx[11])
    share_sum = even + pltpu.roll(odd, 64, 1)
    share_sum = jnp.where(p == 0, share_sum, pltpu.roll(share_sum, 96, 1))
    out = jnp.transpose(share_sum * (scale * STIMULI))
    terms[...] = out[:HALF, : LA * LB]

    a_sub = lax.broadcasted_iota(jnp.int32, (8, 1), 0)
    spread = jnp.broadcast_to(total, (8, 128))
    crosses = spread
    for a in range(1, LA):
        crosses = jnp.where(a_sub == a, pltpu.roll(spread, 128 - a * LB, 1), crosses)
    text_self = pick(32 + jnp.minimum(a_sub, LA - 1), 8)
    vision_self = pltpu.roll(spread, 128 - 40, 1)
    ratio = crosses[:LA, :LB] * (1.0 / jnp.sqrt(text_self[:LA] * vision_self[:LA, :LB]))
    cka[...] = ratio

    for c in range(CHUNKS):
        if c == 0:
            pl.when(p == 1)(lambda: swap(0).wait_send())
        else:
            swap(c).wait_send()
    for axis in range(3):
        for k in (1, 2, 3):
            mean_copy(axis, k).wait_send()

    @pl.loop(p, CHUNKS)
    def _(c):
        part = buf.at[c, pl.ds(0, ALL - ROWS), :]
        pltpu.make_async_copy(part, part, hop_send.at[c]).wait()

    for layer in range(6):
        exchange(layer).wait_send()

    def drain(core):
        for i in range(3):
            q = core * 3 + i
            for j in (2 * q, 2 * q + 1):
                for to in (0, 1):
                    if not (j == OWN and to == core):
                        share(i, j, to).wait_send()

    for core in (0, 1):
        pl.when(p == core)(lambda core=core: drain(core))
    for n in range(15):
        over_plane(n).wait_send()
    for n in range(7):
        over_column(n).wait_send()


def local(text_features, vision_features):
    dma = pltpu.SemaphoreType.DMA
    return pl.pallas_call(
        kernel,
        out_shape=(
            jax.ShapeDtypeStruct((HALF, LA * LB), F32),
            jax.ShapeDtypeStruct((LA, LB), F32),
        ),
        in_specs=[pl.BlockSpec(memory_space=pl.ANY)] * 2,
        out_specs=(pl.BlockSpec(memory_space=pltpu.VMEM), pl.BlockSpec(memory_space=pltpu.VMEM)),
        scratch_shapes=[
            pltpu.VMEM((CHUNKS, ALL, WIDTH), BF16),
            pltpu.VMEM((6, 6, ALL, 128), F32),
            pltpu.VMEM((6, 3, ALL, 128), F32),
            pltpu.VMEM((ALL, WIDTH), BF16),
            pltpu.VMEM((4, CHUNKS, WIDTH), F32),
            pltpu.VMEM((3, 3, CHUNKS, WIDTH), F32),
            pltpu.VMEM((3, 32, 128), F32),
            pltpu.VMEM((16, 128), F32),
            pltpu.VMEM((12, 32, 128), F32),
            pltpu.VMEM((2, 1, 128), F32),
            pltpu.VMEM((16, 1, 128), F32),
            pltpu.VMEM((8, 1, 128), F32),
            dma((CHUNKS,)),
            dma((CHUNKS,)),
            dma((CHUNKS,)),
            dma((3, 3)),
            dma((3, 3)),
            dma((CHUNKS,)),
            dma((CHUNKS, len(BLOCKS))),
            dma((6,)),
            dma((6,)),
            dma((3, 2, 2)),
            dma((12,)),
            dma((15,)),
            dma((16,)),
            dma((7,)),
            dma((8,)),
        ],
        compiler_params=pltpu.CompilerParams(has_side_effects=True, vmem_limit_bytes=60 * 2**20),
    )(text_features, vision_features)


def solution(mesh):
    split = Mesh(mesh.devices.reshape(4, 2, 4, 4), ("row_0", "row_1", "col_0", "col_1"))
    rows = ("row_0", "row_1", "col_0", "col_1")
    placed = (P(None, rows, None), P(None, rows, None))
    return jax.shard_map(local, mesh=split, in_specs=placed, out_specs=(P(rows, None), P()), check_vma=False)
```

```python
import jax
import jax.numpy as jnp
from jax import lax
from jax.experimental import pallas as pl
from jax.experimental.pallas import tpu as pltpu
from jax.sharding import Mesh
from jax.sharding import PartitionSpec as P

STIMULI = 4096
LA, LB = 5, 6
BLOCKS = (
    (0, 1, 0), (0, 0, 2), (3, 0, 0), (2, 0, 0), (1, 3, 0), (1, 1, 1),
    (0, 1, 1), (0, 1, 2), (0, 0, 0), (2, 3, 0), (0, 0, 3), (0, 3, 0),
)
OWN = 8
STRIPS = ((2, 4, 5, 10, 11), (1, 5, 10, 11), (0, 1, 3, 7, 8, 10, 11), (1, 3, 4, 9, 11), (0, 1, 5, 6, 10), (3, 4, 5, 6, 9, 10))
STEPS = ((1, 0, 0), (3, 0, 0), (0, 1, 0), (0, 3, 0), (0, 0, 1), (0, 0, 3))
EDGES = (
    ((8, 0, 2), (8, 2, 1), (8, 10, 5), (8, 11, 3)),
    ((10, 1, 5), (2, 3, 1), (11, 4, 0), (0, 6, 4)),
    ((6, 5, 0), (1, 7, 2), (3, 9, 3)),
)
CHUNKS, WIDTH = 48, 256
PAIRS = CHUNKS // 2
ROWS, HALF = 64, 32
ALL = len(BLOCKS) * ROWS
EARLY, LAG, LATE, PACE = 4, 5, 3, 5
LAST = (3, 10, 17, 19, 21, 23)
F32, BF16 = jnp.float32, jnp.bfloat16
MESH = pl.DeviceIdType.MESH


def kernel(
    text, vision, terms, cka,
    buf, acc, rx, xc, sums, mrx, rs, selfs, pack, rrx, row, ar1, ar2,
    load_sem, swap_send, swap_recv, mean_send, mean_recv, hop_send, hop_recv,
    ex_send, ex_recv, rs_send, rs_recv, ar1_send, ar1_recv, ar2_send, ar2_recv,
):
    y, p = lax.axis_index("row_0"), lax.axis_index("row_1")
    z, x = lax.axis_index("col_0"), lax.axis_index("col_1")

    def at(offset, core):
        dx, dy, dz = offset
        return (lax.rem(y + dy, 4), core, lax.rem(z + dz, 4), lax.rem(x + dx, 4))

    def back(step):
        return tuple((4 - v) % 4 for v in step)

    def remote(src, dst, send, recv, device):
        return pltpu.make_async_remote_copy(
            src_ref=src, dst_ref=dst, send_sem=send, recv_sem=recv, device_id=device, device_id_type=MESH
        )

    other = 1 - p
    here = (0, 0, 0)

    def source(c, core):
        if c < 8:
            return text.at[2, :, pl.ds(pl.multiple_of(core * 1536 + c * WIDTH, WIDTH), WIDTH)]
        if c < 22:
            return text.at[core * 3, :, pl.ds((c - 8) * WIDTH, WIDTH)]
        if c < 36:
            return text.at[core * 3 + 1, :, pl.ds((c - 22) * WIDTH, WIDTH)]
        return vision.at[core * 3 + (c - 36) // 4, :, pl.ds((c - 36) % 4 * WIDTH, WIDTH)]

    first = 2 * p
    mine = pl.ds(pl.multiple_of(OWN * ROWS + p * HALF, HALF), HALF)

    def load(c):
        return pltpu.make_async_copy(source(c, p), buf.at[c, mine, :], load_sem.at[c])

    def swap(c):
        return remote(source(c, other), buf.at[c, mine, :], swap_send.at[c], swap_recv.at[c], at(here, other))

    for c in range(CHUNKS):
        if c < 2:
            pl.when(p == 0)(lambda c=c: load(c).start())
        else:
            load(c).start()

    barrier = pltpu.get_barrier_semaphore()
    greeted = [at(step, p) for step in STEPS]
    greeted.append(at(here, other))
    for device in greeted:
        pl.semaphore_signal(barrier, inc=1, device_id=device, device_id_type=MESH)
    pl.semaphore_wait(barrier, len(greeted))

    for c in range(CHUNKS):
        if c < 2:
            pl.when(p == 1)(lambda c=c: swap(c).start())
        else:
            swap(c).start()

    @pl.loop(0, 36)
    def _(i):
        acc[i // 6, i % 6] = jnp.zeros((ALL, 128), F32)

    rs[...] = jnp.zeros_like(rs)
    selfs[...] = jnp.zeros_like(selfs)

    def hop(edge, c):
        held, becomes, step = edge
        return remote(
            buf.at[c, pl.ds(held * ROWS, ROWS), :],
            buf.at[c, pl.ds(becomes * ROWS, ROWS), :],
            hop_send.at[c],
            hop_recv.at[c, kind[becomes]],
            at(back(STEPS[step]), p),
        )

    inner = [sorted({e[0] for e in EDGES[d]}) for d in range(3)]
    kind = {e[1]: next((d - 1 for d in (1, 2) if e[1] in inner[d]), 2) for d in EDGES for e in d}

    def arrived(which, c):
        part = buf.at[c, pl.ds(0, ROWS * sum(k == which for k in kind.values())), :]
        pltpu.make_async_copy(part, part, hop_recv.at[c, which]).wait()

    def send_own(c):
        for edge in EDGES[0]:
            hop(edge, c).start()

    where = (x, y, z)

    def mean_copy(n):
        axis, second = n // 2, n % 2
        place = list(where)
        place[axis] = 3 - where[axis] if second else where[axis] + 1 - 2 * lax.rem(where[axis], 2)
        device = (place[1], p, place[2], place[0])
        return remote(sums.at[n], mrx.at[n], mean_send.at[n], mean_recv.at[n], device)

    def exchange(layer):
        return remote(
            acc.at[layer, pl.ds(other * 3, 3)], rx.at[layer], ex_send.at[layer], ex_recv.at[layer], at(here, other)
        )

    def compute(k):
        for h in range(2):
            arrived(2, 2 * k + h)
            mean = sums[6, pl.ds(2 * k + h, 1), :] * (1.0 / STIMULI)
            xc[:, h * WIDTH : (h + 1) * WIDTH] = (buf[2 * k + h].astype(F32) - mean).astype(BF16)
        layer = jnp.where(k < 4, 0, jnp.where(k < 11, 1, jnp.where(k < 18, 2, 3 + (k - 18) // 2)))
        for g in range(3):
            tile = lax.dot_general(
                xc[...],
                xc[g * 256 : (g + 1) * 256, :],
                (((1,), (1,)), ((), ())),
                preferred_element_type=F32,
            )
            acc[layer, 2 * g] += tile[:, :128]
            acc[layer, 2 * g + 1] += tile[:, 128:]
        for layer, last in enumerate(LAST):
            pl.when(k == last)(lambda layer=layer: exchange(layer).start())

    def computed(u):
        ready = jnp.minimum((u - LAG - LATE + 1) // 2, u - (6 * PACE - 1))
        return jnp.minimum(jnp.maximum(ready, p), PAIRS)

    def here_now(c):
        part = buf.at[c, mine, :]
        pltpu.make_async_copy(part, part, load_sem.at[c]).wait()
        pltpu.make_async_copy(part, part, swap_recv.at[c]).wait()

    @pl.loop(first, EARLY)
    def _(c):
        here_now(c)
        send_own(c)

    @pl.loop(EARLY, CHUNKS)
    def _(c):
        here_now(c)

    for c in range(CHUNKS):
        total = jnp.sum(buf[c, OWN * ROWS : (OWN + 1) * ROWS, :].astype(F32), axis=0, keepdims=True)
        sums[0, c : c + 1, :] = jnp.where(p == 1, 0.0, total) if c < 2 else total

    mean_copy(0).start()

    @pl.loop(0, CHUNKS + LAG + LATE)
    def _(u):
        for n in range(1, 6):
            pl.when(u == PACE * n)(lambda n=n: mean_copy(n).start())

        @pl.when(u + EARLY < CHUNKS)
        def _():
            send_own(u + EARLY)

        for depth in (1, 2):
            c = u - (depth - 1) * LAG

            @pl.when((c >= first) & (c < CHUNKS))
            def _():
                arrived(depth - 1, c)
                for edge in EDGES[depth]:
                    hop(edge, c).start()

        for n in range(6):

            @pl.when(u == PACE * n + PACE - 1)
            def _():
                mean_copy(n).wait_recv()
                sums[n + 1] = sums[n] + mrx[n]

        @pl.loop(computed(u - 1), computed(u))
        def _(k):
            compute(k)

    for layer in range(6):
        exchange(layer).wait_recv()

    lanes8 = lax.broadcasted_iota(jnp.int32, (8, 128), 1)

    def products(core):
        texts = (0, 1, 2, 3, 4) if core == 0 else (3, 4, 2, 0, 1)
        for i in range(3):
            q = core * 3 + i
            for k in range(3):
                n_text = LA if k == 0 else 0

                def body(r, sums_):
                    s = list(sums_)
                    for block in STRIPS[q]:
                        at_ = pl.ds(pl.multiple_of(block * ROWS + r * 8, 8), 8)
                        t = (
                            acc[1, q, at_, :],
                            acc[2, q, at_, :],
                            acc[0, q, at_, :] + rx[0, i, at_, :],
                            rx[1, i, at_, :],
                            rx[2, i, at_, :],
                        )
                        v = (acc[3 + k, q, at_, :], rx[3 + k, i, at_, :])
                        for a in range(LA):
                            for b in range(2):
                                s[2 * a + b] += t[a] * v[b]
                        for b in range(2):
                            s[10 + b] += v[b] * v[b]
                        for a in range(n_text):
                            s[12 + a] += t[a] * t[a]
                    return tuple(s)

                zero = jnp.zeros((8, 128), F32)
                s = lax.fori_loop(0, 8, body, (zero,) * (12 + n_text))
                visions = (core * 3 + k, (1 - core) * 3 + k)
                for a in range(LA):
                    for b in range(2):
                        n = texts[a] * LB + visions[b]
                        rs[i, n : n + 1, :] = jnp.sum(s[2 * a + b], axis=0, keepdims=True)
                for b in range(2):
                    n = 8 + visions[b]
                    selfs[n : n + 1, :] += jnp.sum(s[10 + b], axis=0, keepdims=True)
                for a in range(n_text):
                    n = texts[a]
                    selfs[n : n + 1, :] += jnp.sum(s[12 + a], axis=0, keepdims=True)

            for j in (2 * q, 2 * q + 1):
                for to in (0, 1):
                    first = j % 2 * ROWS + to * HALF
                    tile = jnp.zeros((8, 128), F32)
                    for g in range(4):
                        turned = rs[i, 8 * g : 8 * g + 8, :]
                        if (g * HALF - first) % 128:
                            turned = pltpu.roll(turned, (g * HALF - first) % 128, 1)
                        tile = jnp.where(lanes8 // HALF == g, turned, tile)
                    if j == OWN and to == core:
                        rrx[j] = tile
                    else:
                        pack[i, j % 2, to] = tile
            for j in (2 * q, 2 * q + 1):
                for to in (0, 1):
                    if not (j == OWN and to == core):
                        share(i, j, to).start()

    def share(i, j, to):
        return remote(pack.at[i, j % 2, to], rrx.at[j], rs_send.at[i, j % 2, to], rs_recv.at[j], at(BLOCKS[j], to))

    for core in (0, 1):
        pl.when(p == core)(lambda core=core: products(core))

    cross = rs[0] + rs[1] + rs[2]
    parts = jnp.concatenate([cross, selfs[...]], axis=0)
    parts = jnp.sum(parts, axis=1, keepdims=True)
    lane = lax.broadcasted_iota(jnp.int32, (48, 128), 1)
    sub = lax.broadcasted_iota(jnp.int32, (48, 128), 0)
    row[0] = jnp.sum(jnp.where(lane == sub, parts, 0.0), axis=0, keepdims=True)

    plane = [(dx, dy) for dx in range(4) for dy in range(4) if dx or dy]
    me1 = x * 4 + y

    def over_plane(n):
        dx, dy = plane[n]
        return remote(row.at[0], ar1.at[me1], ar1_send.at[n], ar1_recv.at[me1], at((dx, dy, 0), p))

    for n in range(15):
        over_plane(n).start()
    ar1[me1] = row[0]
    for dx, dy in plane:
        n = lax.rem(x + dx, 4) * 4 + lax.rem(y + dy, 4)
        pltpu.make_async_copy(ar1.at[n], ar1.at[n], ar1_recv.at[n]).wait()
    row[1] = jnp.sum(ar1[...], axis=0)

    column = [(dz, dc) for dz in range(4) for dc in range(2) if dz or dc]
    me2 = z * 2 + p

    def over_column(n):
        dz, dc = column[n]
        return remote(
            row.at[1], ar2.at[me2], ar2_send.at[n], ar2_recv.at[me2], at((0, 0, dz), other if dc else p)
        )

    for n in range(7):
        over_column(n).start()
    ar2[me2] = row[1]
    for dz, dc in column:
        n = lax.rem(z + dz, 4) * 2 + (other if dc else p)
        pltpu.make_async_copy(ar2.at[n], ar2.at[n], ar2_recv.at[n]).wait()
    total = jnp.sum(ar2[...], axis=0)

    def pick(index, n):
        lanes = lax.broadcasted_iota(jnp.int32, (n, 128), 1)
        return jnp.sum(jnp.where(lanes == index, total, 0.0), axis=1, keepdims=True)

    pair = lax.broadcasted_iota(jnp.int32, (32, 1), 0)
    of_text, of_vision = pair // LB, lax.rem(pair, LB)
    scale = 1.0 / jnp.sqrt(pick(32 + jnp.minimum(of_text, LA - 1), 32) * pick(40 + of_vision, 32))
    for j in range(len(BLOCKS)):
        if j == OWN:
            pl.when(p != OWN // 6)(lambda: pltpu.make_async_copy(rrx.at[OWN], rrx.at[OWN], rs_recv.at[OWN]).wait())
        else:
            pltpu.make_async_copy(rrx.at[j], rrx.at[j], rs_recv.at[j]).wait()
    packed = ((rrx[0] + rrx[1]) + (rrx[2] + rrx[3])) + ((rrx[4] + rrx[5]) + (rrx[6] + rrx[7]))
    packed += (rrx[8] + rrx[9]) + (rrx[10] + rrx[11])
    share_sum = jnp.concatenate([packed] + [pltpu.roll(packed, 128 - g * HALF, 1) for g in (1, 2, 3)], axis=0)
    out = jnp.transpose(share_sum * (scale * STIMULI))
    terms[...] = out[:HALF, : LA * LB]

    a_sub = lax.broadcasted_iota(jnp.int32, (8, 1), 0)
    spread = jnp.broadcast_to(total, (8, 128))
    crosses = spread
    for a in range(1, LA):
        crosses = jnp.where(a_sub == a, pltpu.roll(spread, 128 - a * LB, 1), crosses)
    text_self = pick(32 + jnp.minimum(a_sub, LA - 1), 8)
    vision_self = pltpu.roll(spread, 128 - 40, 1)
    ratio = crosses[:LA, :LB] * (1.0 / jnp.sqrt(text_self[:LA] * vision_self[:LA, :LB]))
    cka[...] = ratio

    for c in range(CHUNKS):
        if c < 2:
            pl.when(p == 1)(lambda c=c: swap(c).wait_send())
        else:
            swap(c).wait_send()
    for n in range(6):
        mean_copy(n).wait_send()

    @pl.loop(first, CHUNKS)
    def _(c):
        part = buf.at[c, pl.ds(0, ALL - ROWS), :]
        pltpu.make_async_copy(part, part, hop_send.at[c]).wait()

    for layer in range(6):
        exchange(layer).wait_send()

    def drain(core):
        for i in range(3):
            q = core * 3 + i
            for j in (2 * q, 2 * q + 1):
                for to in (0, 1):
                    if not (j == OWN and to == core):
                        share(i, j, to).wait_send()

    for core in (0, 1):
        pl.when(p == core)(lambda core=core: drain(core))
    for n in range(15):
        over_plane(n).wait_send()
    for n in range(7):
        over_column(n).wait_send()


def local(text_features, vision_features):
    dma = pltpu.SemaphoreType.DMA
    return pl.pallas_call(
        kernel,
        out_shape=(
            jax.ShapeDtypeStruct((HALF, LA * LB), F32),
            jax.ShapeDtypeStruct((LA, LB), F32),
        ),
        in_specs=[pl.BlockSpec(memory_space=pl.ANY)] * 2,
        out_specs=(pl.BlockSpec(memory_space=pltpu.VMEM), pl.BlockSpec(memory_space=pltpu.VMEM)),
        scratch_shapes=[
            pltpu.VMEM((CHUNKS, ALL, WIDTH), BF16),
            pltpu.VMEM((6, 6, ALL, 128), F32),
            pltpu.VMEM((6, 3, ALL, 128), F32),
            pltpu.VMEM((ALL, 2 * WIDTH), BF16),
            pltpu.VMEM((7, CHUNKS, WIDTH), F32),
            pltpu.VMEM((6, CHUNKS, WIDTH), F32),
            pltpu.VMEM((3, 32, 128), F32),
            pltpu.VMEM((16, 128), F32),
            pltpu.VMEM((3, 2, 2, 8, 128), F32),
            pltpu.VMEM((12, 8, 128), F32),
            pltpu.VMEM((2, 1, 128), F32),
            pltpu.VMEM((16, 1, 128), F32),
            pltpu.VMEM((8, 1, 128), F32),
            dma((CHUNKS,)),
            dma((CHUNKS,)),
            dma((CHUNKS,)),
            dma((6,)),
            dma((6,)),
            dma((CHUNKS,)),
            dma((CHUNKS, 3)),
            dma((6,)),
            dma((6,)),
            dma((3, 2, 2)),
            dma((12,)),
            dma((15,)),
            dma((16,)),
            dma((7,)),
            dma((8,)),
        ],
        compiler_params=pltpu.CompilerParams(collective_id=0, has_side_effects=True, vmem_limit_bytes=60 * 2**20),
    )(text_features, vision_features)


def solution(mesh):
    split = Mesh(mesh.devices.reshape(4, 2, 4, 4), ("row_0", "row_1", "col_0", "col_1"))
    rows = ("row_0", "row_1", "col_0", "col_1")
    placed = (P(None, rows, None), P(None, rows, None))
    return jax.shard_map(local, mesh=split, in_specs=placed, out_specs=(P(rows, None), P()), check_vma=False)
```

```python
import jax
import jax.numpy as jnp
from jax import lax
from jax.experimental import pallas as pl
from jax.experimental.pallas import tpu as pltpu
from jax.sharding import Mesh
from jax.sharding import PartitionSpec as P

STIMULI = 4096
LA, LB = 5, 6
BLOCKS = (
    (0, 1, 0), (0, 0, 2), (3, 0, 0), (2, 0, 0), (1, 3, 0), (1, 1, 1),
    (0, 1, 1), (0, 1, 2), (0, 0, 0), (2, 3, 0), (0, 0, 3), (0, 3, 0),
)
OWN = 8
STRIPS = ((2, 4, 5, 10, 11), (1, 5, 10, 11), (0, 1, 3, 7, 8, 10, 11), (1, 3, 4, 9, 11), (0, 1, 5, 6, 10), (3, 4, 5, 6, 9, 10))
STEPS = ((1, 0, 0), (3, 0, 0), (0, 1, 0), (0, 3, 0), (0, 0, 1), (0, 0, 3))
EDGES = (
    ((8, 0, 2), (8, 2, 1), (8, 10, 5), (8, 11, 3)),
    ((10, 1, 5), (2, 3, 1), (11, 4, 0), (0, 6, 4)),
    ((6, 5, 0), (1, 7, 2), (3, 9, 3)),
)
CHUNKS, WIDTH = 48, 256
PAIRS = CHUNKS // 2
ROWS, HALF = 64, 32
ALL = len(BLOCKS) * ROWS
EARLY, LAG, LATE, PACE = 4, 4, 3, 4
LAST = (3, 10, 17, 19, 21, 23)
F32, BF16 = jnp.float32, jnp.bfloat16
MESH = pl.DeviceIdType.MESH


def kernel(
    text, vision, raw,
    buf, acc, rx, xc, sums, mrx, rs, selfs, pack, rrx, row, ar1, ar2,
    load_sem, swap_send, swap_recv, mean_send, mean_recv, hop_send, hop_recv,
    ex_send, ex_recv, rs_send, rs_recv, ar1_send, ar1_recv, ar2_send, ar2_recv,
):
    y, p = lax.axis_index("row_0"), lax.axis_index("row_1")
    z, x = lax.axis_index("col_0"), lax.axis_index("col_1")

    def at(offset, core):
        dx, dy, dz = offset
        return (lax.rem(y + dy, 4), core, lax.rem(z + dz, 4), lax.rem(x + dx, 4))

    def back(step):
        return tuple((4 - v) % 4 for v in step)

    def remote(src, dst, send, recv, device):
        return pltpu.make_async_remote_copy(
            src_ref=src, dst_ref=dst, send_sem=send, recv_sem=recv, device_id=device, device_id_type=MESH
        )

    other = 1 - p
    here = (0, 0, 0)

    def source(c, core):
        if c < 8:
            return text.at[2, :, pl.ds(pl.multiple_of(core * 1536 + c * WIDTH, WIDTH), WIDTH)]
        if c < 22:
            return text.at[core * 3, :, pl.ds((c - 8) * WIDTH, WIDTH)]
        if c < 36:
            return text.at[core * 3 + 1, :, pl.ds((c - 22) * WIDTH, WIDTH)]
        return vision.at[core * 3 + (c - 36) // 4, :, pl.ds((c - 36) % 4 * WIDTH, WIDTH)]

    first = 2 * p
    mine = pl.ds(pl.multiple_of(OWN * ROWS + p * HALF, HALF), HALF)

    def load(c):
        return pltpu.make_async_copy(source(c, p), buf.at[c, mine, :], load_sem.at[c])

    def swap(c):
        return remote(source(c, other), buf.at[c, mine, :], swap_send.at[c], swap_recv.at[c], at(here, other))

    for c in range(CHUNKS):
        if c < 2:
            pl.when(p == 0)(lambda c=c: load(c).start())
        else:
            load(c).start()

    barrier = pltpu.get_barrier_semaphore()
    greeted = [at(step, p) for step in STEPS]
    greeted.append(at(here, other))
    for device in greeted:
        pl.semaphore_signal(barrier, inc=1, device_id=device, device_id_type=MESH)
    pl.semaphore_wait(barrier, len(greeted))

    for c in range(CHUNKS):
        if c < 2:
            pl.when(p == 1)(lambda c=c: swap(c).start())
        else:
            swap(c).start()

    @pl.loop(0, 36)
    def _(i):
        acc[i // 6, i % 6] = jnp.zeros((ALL, 128), F32)

    rs[...] = jnp.zeros_like(rs)
    selfs[...] = jnp.zeros_like(selfs)

    def hop(edge, c):
        held, becomes, step = edge
        return remote(
            buf.at[c, pl.ds(held * ROWS, ROWS), :],
            buf.at[c, pl.ds(becomes * ROWS, ROWS), :],
            hop_send.at[c],
            hop_recv.at[c, kind[becomes]],
            at(back(STEPS[step]), p),
        )

    inner = [sorted({e[0] for e in EDGES[d]}) for d in range(3)]
    kind = {e[1]: next((d - 1 for d in (1, 2) if e[1] in inner[d]), 2) for d in EDGES for e in d}

    def arrived(which, c):
        part = buf.at[c, pl.ds(0, ROWS * sum(k == which for k in kind.values())), :]
        pltpu.make_async_copy(part, part, hop_recv.at[c, which]).wait()

    def send_own(c):
        for edge in EDGES[0]:
            hop(edge, c).start()

    where = (x, y, z)

    def mean_copy(n):
        axis, second = n // 2, n % 2
        place = list(where)
        place[axis] = 3 - where[axis] if second else where[axis] + 1 - 2 * lax.rem(where[axis], 2)
        device = (place[1], p, place[2], place[0])
        return remote(sums.at[n], mrx.at[n], mean_send.at[n], mean_recv.at[n], device)

    def exchange(layer):
        for core in (0, 1):

            @pl.when(p == core)
            def _():
                for i in range(3):
                    q = (1 - core) * 3 + i
                    for block in STRIPS[q]:
                        strip = pl.ds(block * ROWS, ROWS)
                        remote(
                            acc.at[layer, q, strip],
                            rx.at[layer, i, strip],
                            ex_send.at[layer],
                            ex_recv.at[layer],
                            at(here, other),
                        ).start()

    def exchanged(sem):
        part = acc.at[0, pl.ds(0, 2), pl.ds(0, 8 * ROWS)]
        pltpu.make_async_copy(part, part, sem).wait()

    def products(core, k):
        texts = (0, 1, 2, 3, 4) if core == 0 else (3, 4, 2, 0, 1)
        for i in range(3):
            q = core * 3 + i
            n_text = LA if k == 0 else 0

            def body(r, sums_):
                s = list(sums_)
                for block in STRIPS[q]:
                    at_ = pl.ds(pl.multiple_of(block * ROWS + r * 8, 8), 8)
                    t = (
                        acc[1, q, at_, :],
                        acc[2, q, at_, :],
                        acc[0, q, at_, :] + rx[0, i, at_, :],
                        rx[1, i, at_, :],
                        rx[2, i, at_, :],
                    )
                    v = (acc[3 + k, q, at_, :], rx[3 + k, i, at_, :])
                    for a in range(LA):
                        for b in range(2):
                            s[2 * a + b] += t[a] * v[b]
                    for b in range(2):
                        s[10 + b] += v[b] * v[b]
                    for a in range(n_text):
                        s[12 + a] += t[a] * t[a]
                return tuple(s)

            zero = jnp.zeros((8, 128), F32)
            s = lax.fori_loop(0, 8, body, (zero,) * (12 + n_text))
            visions = (core * 3 + k, (1 - core) * 3 + k)
            for a in range(LA):
                for b in range(2):
                    n = texts[a] * LB + visions[b]
                    rs[i, n : n + 1, :] = jnp.sum(s[2 * a + b], axis=0, keepdims=True)
            for b in range(2):
                n = 8 + visions[b]
                selfs[n : n + 1, :] += jnp.sum(s[10 + b], axis=0, keepdims=True)
            for a in range(n_text):
                n = texts[a]
                selfs[n : n + 1, :] += jnp.sum(s[12 + a], axis=0, keepdims=True)

    def compute(k):
        for h in range(2):
            arrived(2, 2 * k + h)
            mean = sums[6, pl.ds(2 * k + h, 1), :] * (1.0 / STIMULI)
            xc[:, h * WIDTH : (h + 1) * WIDTH] = (buf[2 * k + h].astype(F32) - mean).astype(BF16)
        layer = jnp.where(k < 4, 0, jnp.where(k < 11, 1, jnp.where(k < 18, 2, 3 + (k - 18) // 2)))
        for g in range(3):
            blocks = sorted({*STRIPS[2 * g], *STRIPS[2 * g + 1]})
            tile = lax.dot_general(
                jnp.concatenate([xc[b * ROWS : (b + 1) * ROWS, :] for b in blocks], axis=0),
                xc[g * 256 : (g + 1) * 256, :],
                (((1,), (1,)), ((), ())),
                preferred_element_type=F32,
            )
            for n, b in enumerate(blocks):
                strip = slice(b * ROWS, (b + 1) * ROWS)
                for h in range(2):
                    if b in STRIPS[2 * g + h]:
                        acc[layer, 2 * g + h, strip] += tile[n * ROWS : (n + 1) * ROWS, h * 128 : (h + 1) * 128]
        for layer, last in enumerate(LAST):
            pl.when(k == last)(lambda layer=layer: exchange(layer))
        for n in (0, 1):

            @pl.when(k == LAST[3 + n] + 1)
            def _():
                for layer in (0, 1, 2, 3) if n == 0 else (4,):
                    exchanged(ex_recv.at[layer])
                for core in (0, 1):
                    pl.when(p == core)(lambda core=core: products(core, n))


    def computed(u):
        ready = jnp.minimum((u - LAG - LATE + 1) // 2, u - (6 * PACE - 1))
        return jnp.minimum(jnp.maximum(ready, p), PAIRS)

    def here_now(c):
        part = buf.at[c, mine, :]
        pltpu.make_async_copy(part, part, load_sem.at[c]).wait()
        pltpu.make_async_copy(part, part, swap_recv.at[c]).wait()

    def send_half(c, core):
        for held, becomes, step in EDGES[0]:
            rows = [pl.ds(pl.multiple_of(b * ROWS + core * HALF, HALF), HALF) for b in (held, becomes)]
            remote(
                buf.at[c, rows[0], :],
                buf.at[c, rows[1], :],
                hop_send.at[c],
                hop_recv.at[c, kind[becomes]],
                at(back(STEPS[step]), p),
            ).start()

    @pl.loop(first, EARLY)
    def _(c):
        part = buf.at[c, mine, :]
        pltpu.make_async_copy(part, part, load_sem.at[c]).wait()
        send_half(c, p)

    @pl.loop(first, EARLY)
    def _(c):
        part = buf.at[c, mine, :]
        pltpu.make_async_copy(part, part, swap_recv.at[c]).wait()
        send_half(c, other)

    @pl.loop(EARLY, CHUNKS)
    def _(c):
        here_now(c)

    for c in range(CHUNKS):
        total = jnp.sum(buf[c, OWN * ROWS : (OWN + 1) * ROWS, :].astype(F32), axis=0, keepdims=True)
        sums[0, c : c + 1, :] = jnp.where(p == 1, 0.0, total) if c < 2 else total

    mean_copy(0).start()

    @pl.loop(0, CHUNKS + LAG + LATE)
    def _(u):
        for n in range(1, 6):
            pl.when(u == PACE * n)(lambda n=n: mean_copy(n).start())

        @pl.when(u + EARLY < CHUNKS)
        def _():
            send_own(u + EARLY)

        for depth in (1, 2):
            c = u - (depth - 1) * LAG

            @pl.when((c >= first) & (c < CHUNKS))
            def _():
                arrived(depth - 1, c)
                for edge in EDGES[depth]:
                    hop(edge, c).start()

        for n in range(6):

            @pl.when(u == PACE * n + PACE - 1)
            def _():
                mean_copy(n).wait_recv()
                sums[n + 1] = sums[n] + mrx[n]

        @pl.loop(computed(u - 1), computed(u))
        def _(k):
            compute(k)

    exchanged(ex_recv.at[5])

    lanes8 = lax.broadcasted_iota(jnp.int32, (8, 128), 1)

    def deliver(core):
        for i in range(3):
            q = core * 3 + i
            for j in (2 * q, 2 * q + 1):
                for to in (0, 1):
                    first = j % 2 * ROWS + to * HALF
                    tile = jnp.zeros((8, 128), F32)
                    for g in range(4):
                        turned = rs[i, 8 * g : 8 * g + 8, :]
                        if (g * HALF - first) % 128:
                            turned = pltpu.roll(turned, (g * HALF - first) % 128, 1)
                        tile = jnp.where(lanes8 // HALF == g, turned, tile)
                    if j == OWN and to == core:
                        rrx[j] = tile
                    else:
                        pack[i, j % 2, to] = tile
            for j in (2 * q, 2 * q + 1):
                for to in (0, 1):
                    if not (j == OWN and to == core):
                        share(i, j, to).start()

    def share(i, j, to):
        return remote(pack.at[i, j % 2, to], rrx.at[j], rs_send.at[i, j % 2, to], rs_recv.at[j], at(BLOCKS[j], to))

    for core in (0, 1):

        @pl.when(p == core)
        def _():
            products(core, 2)

    cross = rs[0] + rs[1] + rs[2]
    parts = jnp.concatenate([cross, selfs[...]], axis=0)
    parts = jnp.sum(parts, axis=1, keepdims=True)
    lane = lax.broadcasted_iota(jnp.int32, (48, 128), 1)
    sub = lax.broadcasted_iota(jnp.int32, (48, 128), 0)
    row[0] = jnp.sum(jnp.where(lane == sub, parts, 0.0), axis=0, keepdims=True)

    plane = [(dx, dy) for dx in range(4) for dy in range(4) if dx or dy]
    me1 = x * 4 + y

    def over_plane(n):
        dx, dy = plane[n]
        return remote(row.at[0], ar1.at[me1], ar1_send.at[n], ar1_recv.at[me1], at((dx, dy, 0), p))

    for n in range(15):
        over_plane(n).start()
    for core in (0, 1):
        pl.when(p == core)(lambda core=core: deliver(core))
    ar1[me1] = row[0]
    for dx, dy in plane:
        n = lax.rem(x + dx, 4) * 4 + lax.rem(y + dy, 4)
        pltpu.make_async_copy(ar1.at[n], ar1.at[n], ar1_recv.at[n]).wait()
    row[1] = jnp.sum(ar1[...], axis=0)

    column = [(dz, dc) for dz in range(4) for dc in range(2) if dz or dc]
    me2 = z * 2 + p

    def over_column(n):
        dz, dc = column[n]
        return remote(
            row.at[1], ar2.at[me2], ar2_send.at[n], ar2_recv.at[me2], at((0, 0, dz), other if dc else p)
        )

    for n in range(7):
        over_column(n).start()
    ar2[me2] = row[1]
    for dz, dc in column:
        n = lax.rem(z + dz, 4) * 2 + (other if dc else p)
        pltpu.make_async_copy(ar2.at[n], ar2.at[n], ar2_recv.at[n]).wait()
    total = jnp.sum(ar2[...], axis=0)

    def pick(index, n):
        lanes = lax.broadcasted_iota(jnp.int32, (n, 128), 1)
        return jnp.sum(jnp.where(lanes == index, total, 0.0), axis=1, keepdims=True)

    pair = lax.broadcasted_iota(jnp.int32, (32, 1), 0)
    of_text, of_vision = pair // LB, lax.rem(pair, LB)
    scale = 1.0 / jnp.sqrt(pick(32 + jnp.minimum(of_text, LA - 1), 32) * pick(40 + of_vision, 32))
    for j in range(len(BLOCKS)):
        if j == OWN:
            pl.when(p != OWN // 6)(lambda: pltpu.make_async_copy(rrx.at[OWN], rrx.at[OWN], rs_recv.at[OWN]).wait())
        else:
            pltpu.make_async_copy(rrx.at[j], rrx.at[j], rs_recv.at[j]).wait()
    packed = ((rrx[0] + rrx[1]) + (rrx[2] + rrx[3])) + ((rrx[4] + rrx[5]) + (rrx[6] + rrx[7]))
    packed += (rrx[8] + rrx[9]) + (rrx[10] + rrx[11])
    share_sum = jnp.concatenate([packed] + [pltpu.roll(packed, 128 - g * HALF, 1) for g in (1, 2, 3)], axis=0)
    raw[0:32] = share_sum * (scale * STIMULI)

    a_sub = lax.broadcasted_iota(jnp.int32, (8, 1), 0)
    spread = jnp.broadcast_to(total, (8, 128))
    crosses = spread
    for a in range(1, LA):
        crosses = jnp.where(a_sub == a, pltpu.roll(spread, 128 - a * LB, 1), crosses)
    text_self = pick(32 + jnp.minimum(a_sub, LA - 1), 8)
    vision_self = pltpu.roll(spread, 128 - 40, 1)
    raw[32:37, :LB] = crosses[:LA, :LB] * (1.0 / jnp.sqrt(text_self[:LA] * vision_self[:LA, :LB]))

    for c in range(CHUNKS):
        if c < 2:
            pl.when(p == 1)(lambda c=c: swap(c).wait_send())
        else:
            swap(c).wait_send()
    for n in range(6):
        mean_copy(n).wait_send()

    @pl.loop(first, CHUNKS)
    def _(c):
        part = buf.at[c, pl.ds(0, ALL - ROWS), :]
        pltpu.make_async_copy(part, part, hop_send.at[c]).wait()

    for layer in range(6):
        exchanged(ex_send.at[layer])

    def drain(core):
        for i in range(3):
            q = core * 3 + i
            for j in (2 * q, 2 * q + 1):
                for to in (0, 1):
                    if not (j == OWN and to == core):
                        share(i, j, to).wait_send()

    for core in (0, 1):
        pl.when(p == core)(lambda core=core: drain(core))
    for n in range(15):
        over_plane(n).wait_send()
    for n in range(7):
        over_column(n).wait_send()


def write(raw, terms, cka):
    terms[...] = jnp.transpose(raw[0:32])[:HALF, : LA * LB]
    cka[...] = raw[32:37, :LB]


def local(text_features, vision_features):
    dma = pltpu.SemaphoreType.DMA
    raw = pl.pallas_call(
        kernel,
        out_shape=jax.ShapeDtypeStruct((40, 128), F32),
        in_specs=[pl.BlockSpec(memory_space=pl.ANY)] * 2,
        out_specs=pl.BlockSpec(memory_space=pltpu.VMEM),
        scratch_shapes=[
            pltpu.VMEM((CHUNKS, ALL, WIDTH), BF16),
            pltpu.VMEM((6, 6, ALL, 128), F32),
            pltpu.VMEM((6, 3, ALL, 128), F32),
            pltpu.VMEM((ALL, 2 * WIDTH), BF16),
            pltpu.VMEM((7, CHUNKS, WIDTH), F32),
            pltpu.VMEM((6, CHUNKS, WIDTH), F32),
            pltpu.VMEM((3, 32, 128), F32),
            pltpu.VMEM((16, 128), F32),
            pltpu.VMEM((3, 2, 2, 8, 128), F32),
            pltpu.VMEM((12, 8, 128), F32),
            pltpu.VMEM((2, 1, 128), F32),
            pltpu.VMEM((16, 1, 128), F32),
            pltpu.VMEM((8, 1, 128), F32),
            dma((CHUNKS,)),
            dma((CHUNKS,)),
            dma((CHUNKS,)),
            dma((6,)),
            dma((6,)),
            dma((CHUNKS,)),
            dma((CHUNKS, 3)),
            dma((6,)),
            dma((6,)),
            dma((3, 2, 2)),
            dma((12,)),
            dma((15,)),
            dma((16,)),
            dma((7,)),
            dma((8,)),
        ],
        compiler_params=pltpu.CompilerParams(collective_id=0, has_side_effects=True, vmem_limit_bytes=60 * 2**20),
    )(text_features, vision_features)
    return pl.pallas_call(
        write,
        out_shape=(
            jax.ShapeDtypeStruct((HALF, LA * LB), F32),
            jax.ShapeDtypeStruct((LA, LB), F32),
        ),
        in_specs=[pl.BlockSpec(memory_space=pltpu.VMEM)],
        out_specs=(pl.BlockSpec(memory_space=pltpu.VMEM),) * 2,
    )(raw)


def solution(mesh):
    split = Mesh(mesh.devices.reshape(4, 2, 4, 4), ("row_0", "row_1", "col_0", "col_1"))
    rows = ("row_0", "row_1", "col_0", "col_1")
    placed = (P(None, rows, None), P(None, rows, None))
    return jax.shard_map(local, mesh=split, in_specs=placed, out_specs=(P(rows, None), P()), check_vma=False)
```

```python
import jax
import jax.numpy as jnp
from jax import lax
from jax.experimental import pallas as pl
from jax.experimental.pallas import tpu as pltpu
from jax.sharding import Mesh
from jax.sharding import PartitionSpec as P

STIMULI = 4096
LA, LB = 5, 6
BLOCKS = (
    (0, 1, 0), (0, 0, 2), (3, 0, 0), (2, 0, 0), (1, 3, 0), (1, 1, 1),
    (0, 1, 1), (0, 1, 2), (0, 0, 0), (2, 3, 0), (0, 0, 3), (0, 3, 0),
)
OWN = 8
STRIPS = ((2, 4, 5, 10, 11), (1, 5, 10, 11), (0, 1, 3, 7, 8, 10, 11), (1, 3, 4, 9, 11), (0, 1, 5, 6, 10), (3, 4, 5, 6, 9, 10))
STEPS = ((1, 0, 0), (3, 0, 0), (0, 1, 0), (0, 3, 0), (0, 0, 1), (0, 0, 3))
EDGES = (
    ((8, 0, 2), (8, 2, 1), (8, 10, 5), (8, 11, 3)),
    ((10, 1, 5), (2, 3, 1), (11, 4, 0), (0, 6, 4)),
    ((6, 5, 0), (1, 7, 2), (3, 9, 3)),
)
CHUNKS, WIDTH = 48, 256
PAIRS = CHUNKS // 2
ROWS, HALF = 64, 32
ALL = len(BLOCKS) * ROWS
EARLY, LAG, LATE, PACE = 4, 4, 3, 4
LAST = (3, 10, 17, 19, 21, 23)
F32, BF16 = jnp.float32, jnp.bfloat16
MESH = pl.DeviceIdType.MESH


def kernel(
    text, vision, raw,
    buf, acc, rx, xc, sums, mrx, rs, selfs, pack, rrx, row, ar1, ar2,
    load_sem, swap_send, swap_recv, mean_send, mean_recv, hop_send, hop_recv, last_recv,
    ex_send, ex_recv, rs_send, rs_recv, ar1_send, ar1_recv, ar2_send, ar2_recv,
):
    y, p = lax.axis_index("row_0"), lax.axis_index("row_1")
    z, x = lax.axis_index("col_0"), lax.axis_index("col_1")

    def at(offset, core):
        dx, dy, dz = offset
        return (lax.rem(y + dy, 4), core, lax.rem(z + dz, 4), lax.rem(x + dx, 4))

    def back(step):
        return tuple((4 - v) % 4 for v in step)

    def remote(src, dst, send, recv, device):
        return pltpu.make_async_remote_copy(
            src_ref=src, dst_ref=dst, send_sem=send, recv_sem=recv, device_id=device, device_id_type=MESH
        )

    other = 1 - p
    here = (0, 0, 0)

    def source(c, core):
        if c < 8:
            return text.at[2, :, pl.ds(pl.multiple_of(core * 1536 + c * WIDTH, WIDTH), WIDTH)]
        if c < 22:
            return text.at[core * 3, :, pl.ds((c - 8) * WIDTH, WIDTH)]
        if c < 36:
            return text.at[core * 3 + 1, :, pl.ds((c - 22) * WIDTH, WIDTH)]
        return vision.at[core * 3 + (c - 36) // 4, :, pl.ds((c - 36) % 4 * WIDTH, WIDTH)]

    first = 2 * p
    mine = pl.ds(pl.multiple_of(OWN * ROWS + p * HALF, HALF), HALF)

    def load(c):
        return pltpu.make_async_copy(source(c, p), buf.at[c, mine, :], load_sem.at[min(c, EARLY)])

    def swap(c):
        return remote(source(c, other), buf.at[c, mine, :], swap_send, swap_recv.at[min(c, EARLY)], at(here, other))

    for c in range(CHUNKS):
        if c < 2:
            pl.when(p == 0)(lambda c=c: load(c).start())
        else:
            load(c).start()

    barrier = pltpu.get_barrier_semaphore()
    greeted = [at(step, p) for step in STEPS]
    greeted.append(at(here, other))
    for device in greeted:
        pl.semaphore_signal(barrier, inc=1, device_id=device, device_id_type=MESH)
    pl.semaphore_wait(barrier, len(greeted))

    for c in range(CHUNKS):
        if c < 2:
            pl.when(p == 1)(lambda c=c: swap(c).start())
        else:
            swap(c).start()

    @pl.loop(0, 36)
    def _(i):
        acc[i // 6, i % 6] = jnp.zeros((ALL, 128), F32)

    rs[...] = jnp.zeros_like(rs)
    selfs[...] = jnp.zeros_like(selfs)

    def hop(edge, c):
        held, becomes, step = edge
        return remote(
            buf.at[c, pl.ds(held * ROWS, ROWS), :],
            buf.at[c, pl.ds(becomes * ROWS, ROWS), :],
            hop_send,
            last_recv.at[c // 2] if kind[becomes] == 2 else hop_recv.at[kind[becomes], c],
            at(back(STEPS[step]), p),
        )

    inner = [sorted({e[0] for e in EDGES[d]}) for d in range(3)]
    kind = {e[1]: next((d - 1 for d in (1, 2) if e[1] in inner[d]), 2) for d in EDGES for e in d}

    def arrived(which, c):
        part = buf.at[c, pl.ds(0, ROWS * sum(k == which for k in kind.values())), :]
        pltpu.make_async_copy(part, part, hop_recv.at[which, c]).wait()

    def arrived_pair(k):
        part = buf.at[pl.ds(2 * k, 2), pl.ds(0, ROWS * sum(k == 2 for k in kind.values())), :]
        pltpu.make_async_copy(part, part, last_recv.at[k]).wait()

    def send_own(c):
        for edge in EDGES[0]:
            hop(edge, c).start()

    where = (x, y, z)

    def mean_copy(n):
        axis, second = n // 2, n % 2
        place = list(where)
        place[axis] = 3 - where[axis] if second else where[axis] + 1 - 2 * lax.rem(where[axis], 2)
        device = (place[1], p, place[2], place[0])
        return remote(sums.at[n], mrx.at[n], mean_send, mean_recv.at[n], device)

    def exchange(layer):
        for core in (0, 1):

            @pl.when(p == core)
            def _():
                for i in range(3):
                    q = (1 - core) * 3 + i
                    for block in STRIPS[q]:
                        strip = pl.ds(block * ROWS, ROWS)
                        remote(
                            acc.at[layer, q, strip],
                            rx.at[layer, i, strip],
                            ex_send,
                            ex_recv.at[layer],
                            at(here, other),
                        ).start()

    def exchanged(sem):
        part = acc.at[0, pl.ds(0, 2), pl.ds(0, 8 * ROWS)]
        pltpu.make_async_copy(part, part, sem).wait()

    def products(core, k):
        texts = (0, 1, 2, 3, 4) if core == 0 else (3, 4, 2, 0, 1)
        for i in range(3):
            q = core * 3 + i
            n_text = LA if k == 0 else 0

            def body(r, sums_):
                s = list(sums_)
                for block in STRIPS[q]:
                    at_ = pl.ds(pl.multiple_of(block * ROWS + r * 8, 8), 8)
                    t = (
                        acc[1, q, at_, :],
                        acc[2, q, at_, :],
                        acc[0, q, at_, :] + rx[0, i, at_, :],
                        rx[1, i, at_, :],
                        rx[2, i, at_, :],
                    )
                    v = (acc[3 + k, q, at_, :], rx[3 + k, i, at_, :])
                    for a in range(LA):
                        for b in range(2):
                            s[2 * a + b] += t[a] * v[b]
                    for b in range(2):
                        s[10 + b] += v[b] * v[b]
                    for a in range(n_text):
                        s[12 + a] += t[a] * t[a]
                return tuple(s)

            zero = jnp.zeros((8, 128), F32)
            s = lax.fori_loop(0, 8, body, (zero,) * (12 + n_text))
            visions = (core * 3 + k, (1 - core) * 3 + k)
            for a in range(LA):
                for b in range(2):
                    n = texts[a] * LB + visions[b]
                    rs[i, n : n + 1, :] = jnp.sum(s[2 * a + b], axis=0, keepdims=True)
            for b in range(2):
                n = 8 + visions[b]
                selfs[n : n + 1, :] += jnp.sum(s[10 + b], axis=0, keepdims=True)
            for a in range(n_text):
                n = texts[a]
                selfs[n : n + 1, :] += jnp.sum(s[12 + a], axis=0, keepdims=True)

    def compute(k):
        arrived_pair(k)
        for h in range(2):
            mean = sums[6, pl.ds(2 * k + h, 1), :] * (1.0 / STIMULI)
            xc[:, h * WIDTH : (h + 1) * WIDTH] = (buf[2 * k + h].astype(F32) - mean).astype(BF16)
        layer = jnp.where(k < 4, 0, jnp.where(k < 11, 1, jnp.where(k < 18, 2, 3 + (k - 18) // 2)))
        for g in range(3):
            blocks = sorted({*STRIPS[2 * g], *STRIPS[2 * g + 1]})
            tile = lax.dot_general(
                jnp.concatenate([xc[b * ROWS : (b + 1) * ROWS, :] for b in blocks], axis=0),
                xc[g * 256 : (g + 1) * 256, :],
                (((1,), (1,)), ((), ())),
                preferred_element_type=F32,
            )
            for n, b in enumerate(blocks):
                strip = slice(b * ROWS, (b + 1) * ROWS)
                for h in range(2):
                    if b in STRIPS[2 * g + h]:
                        acc[layer, 2 * g + h, strip] += tile[n * ROWS : (n + 1) * ROWS, h * 128 : (h + 1) * 128]
        for layer, last in enumerate(LAST):
            pl.when(k == last)(lambda layer=layer: exchange(layer))
        for n in (0, 1):

            @pl.when(k == LAST[3 + n] + 1)
            def _():
                for layer in (0, 1, 2, 3) if n == 0 else (4,):
                    exchanged(ex_recv.at[layer])
                for core in (0, 1):
                    pl.when(p == core)(lambda core=core: products(core, n))


    def computed(u):
        ready = jnp.minimum((u - LAG - LATE + 1) // 2, u - (6 * PACE - 1))
        return jnp.minimum(jnp.maximum(ready, p), PAIRS)

    def send_half(c, core):
        for held, becomes, step in EDGES[0]:
            rows = [pl.ds(pl.multiple_of(b * ROWS + core * HALF, HALF), HALF) for b in (held, becomes)]
            remote(
                buf.at[c, rows[0], :],
                buf.at[c, rows[1], :],
                hop_send,
                last_recv.at[c // 2] if kind[becomes] == 2 else hop_recv.at[kind[becomes], c],
                at(back(STEPS[step]), p),
            ).start()

    @pl.loop(first, EARLY)
    def _(c):
        part = buf.at[c, mine, :]
        pltpu.make_async_copy(part, part, load_sem.at[c]).wait()
        send_half(c, p)

    @pl.loop(first, EARLY)
    def _(c):
        part = buf.at[c, mine, :]
        pltpu.make_async_copy(part, part, swap_recv.at[c]).wait()
        send_half(c, other)

    rest = buf.at[pl.ds(EARLY, CHUNKS - EARLY), mine, :]
    pltpu.make_async_copy(rest, rest, load_sem.at[EARLY]).wait()
    pltpu.make_async_copy(rest, rest, swap_recv.at[EARLY]).wait()

    for c in range(CHUNKS):
        total = jnp.sum(buf[c, OWN * ROWS : (OWN + 1) * ROWS, :].astype(F32), axis=0, keepdims=True)
        sums[0, c : c + 1, :] = jnp.where(p == 1, 0.0, total) if c < 2 else total

    mean_copy(0).start()

    @pl.loop(0, CHUNKS + LAG + LATE)
    def _(u):
        for n in range(1, 6):
            pl.when(u == PACE * n)(lambda n=n: mean_copy(n).start())

        @pl.when(u + EARLY < CHUNKS)
        def _():
            send_own(u + EARLY)

        for depth in (2, 1):
            c = u - (depth - 1) * LAG

            @pl.when((c >= first) & (c < CHUNKS))
            def _():
                arrived(depth - 1, c)
                for edge in EDGES[depth]:
                    hop(edge, c).start()

        for n in range(6):

            @pl.when(u == PACE * n + PACE - 1)
            def _():
                mean_copy(n).wait_recv()
                sums[n + 1] = sums[n] + mrx[n]

        @pl.loop(computed(u - 1), computed(u))
        def _(k):
            compute(k)

    exchanged(ex_recv.at[5])

    lanes8 = lax.broadcasted_iota(jnp.int32, (8, 128), 1)

    def deliver(core):
        for i in range(3):
            q = core * 3 + i
            for j in (2 * q, 2 * q + 1):
                for to in (0, 1):
                    first = j % 2 * ROWS + to * HALF
                    tile = jnp.zeros((8, 128), F32)
                    for g in range(4):
                        turned = rs[i, 8 * g : 8 * g + 8, :]
                        if (g * HALF - first) % 128:
                            turned = pltpu.roll(turned, (g * HALF - first) % 128, 1)
                        tile = jnp.where(lanes8 // HALF == g, turned, tile)
                    if j == OWN and to == core:
                        rrx[j] = tile
                    else:
                        pack[i, j % 2, to] = tile
            for j in (2 * q, 2 * q + 1):
                for to in (0, 1):
                    if not (j == OWN and to == core):
                        share(i, j, to).start()

    def share(i, j, to):
        return remote(pack.at[i, j % 2, to], rrx.at[j], rs_send, rs_recv, at(BLOCKS[j], to))

    for core in (0, 1):

        @pl.when(p == core)
        def _():
            products(core, 2)

    cross = rs[0] + rs[1] + rs[2]
    parts = jnp.concatenate([cross, selfs[...]], axis=0)
    parts = jnp.sum(parts, axis=1, keepdims=True)
    lane = lax.broadcasted_iota(jnp.int32, (48, 128), 1)
    sub = lax.broadcasted_iota(jnp.int32, (48, 128), 0)
    row[0] = jnp.sum(jnp.where(lane == sub, parts, 0.0), axis=0, keepdims=True)

    plane = [(dx, dy) for dx in range(4) for dy in range(4) if dx or dy]
    me1 = x * 4 + y

    def over_plane(n):
        dx, dy = plane[n]
        return remote(row.at[0], ar1.at[me1], ar1_send, ar1_recv, at((dx, dy, 0), p))

    for n in range(15):
        over_plane(n).start()
    for core in (0, 1):
        pl.when(p == core)(lambda core=core: deliver(core))
    ar1[me1] = row[0]
    others1 = ar1.at[pl.ds(0, 15)]
    pltpu.make_async_copy(others1, others1, ar1_recv).wait()
    row[1] = jnp.sum(ar1[...], axis=0)

    column = [(dz, dc) for dz in range(4) for dc in range(2) if dz or dc]
    me2 = z * 2 + p

    def over_column(n):
        dz, dc = column[n]
        return remote(
            row.at[1], ar2.at[me2], ar2_send, ar2_recv, at((0, 0, dz), other if dc else p)
        )

    for n in range(7):
        over_column(n).start()
    ar2[me2] = row[1]
    others2 = ar2.at[pl.ds(0, 7)]
    pltpu.make_async_copy(others2, others2, ar2_recv).wait()
    total = jnp.sum(ar2[...], axis=0)

    def pick(index, n):
        lanes = lax.broadcasted_iota(jnp.int32, (n, 128), 1)
        return jnp.sum(jnp.where(lanes == index, total, 0.0), axis=1, keepdims=True)

    pair = lax.broadcasted_iota(jnp.int32, (32, 1), 0)
    of_text, of_vision = pair // LB, lax.rem(pair, LB)
    scale = 1.0 / jnp.sqrt(pick(32 + jnp.minimum(of_text, LA - 1), 32) * pick(40 + of_vision, 32))
    def tiles(core, sem):
        part = rrx.at[pl.ds(0, len(BLOCKS) - (core == OWN // 6))]
        pltpu.make_async_copy(part, part, sem).wait()

    for core in (0, 1):
        pl.when(p == core)(lambda core=core: tiles(core, rs_recv))
    packed = ((rrx[0] + rrx[1]) + (rrx[2] + rrx[3])) + ((rrx[4] + rrx[5]) + (rrx[6] + rrx[7]))
    packed += (rrx[8] + rrx[9]) + (rrx[10] + rrx[11])
    share_sum = jnp.concatenate([packed] + [pltpu.roll(packed, 128 - g * HALF, 1) for g in (1, 2, 3)], axis=0)
    raw[0:32] = share_sum * (scale * STIMULI)

    a_sub = lax.broadcasted_iota(jnp.int32, (8, 1), 0)
    spread = jnp.broadcast_to(total, (8, 128))
    crosses = spread
    for a in range(1, LA):
        crosses = jnp.where(a_sub == a, pltpu.roll(spread, 128 - a * LB, 1), crosses)
    text_self = pick(32 + jnp.minimum(a_sub, LA - 1), 8)
    vision_self = pltpu.roll(spread, 128 - 40, 1)
    raw[32:37, :LB] = crosses[:LA, :LB] * (1.0 / jnp.sqrt(text_self[:LA] * vision_self[:LA, :LB]))

    def drain(core):
        crossed = buf.at[pl.ds(0, CHUNKS - 2 * (1 - core)), pl.ds(0, HALF), :]
        hopped = buf.at[pl.ds(0, CHUNKS - 2 * core), pl.ds(0, ALL - ROWS), :]
        pltpu.make_async_copy(crossed, crossed, swap_send).wait()
        pltpu.make_async_copy(hopped, hopped, hop_send).wait()
        tiles(core, rs_send)

    for core in (0, 1):
        pl.when(p == core)(lambda core=core: drain(core))
    means = sums.at[pl.ds(0, 6)]
    pltpu.make_async_copy(means, means, mean_send).wait()
    strips = acc.at[pl.ds(0, 6), pl.ds(0, 2), pl.ds(0, 8 * ROWS)]
    pltpu.make_async_copy(strips, strips, ex_send).wait()
    pltpu.make_async_copy(others1, others1, ar1_send).wait()
    pltpu.make_async_copy(others2, others2, ar2_send).wait()


def write(raw, terms, cka):
    terms[...] = jnp.transpose(raw[0:32])[:HALF, : LA * LB]
    cka[...] = raw[32:37, :LB]


def local(text_features, vision_features):
    dma = pltpu.SemaphoreType.DMA
    raw = pl.pallas_call(
        kernel,
        out_shape=jax.ShapeDtypeStruct((40, 128), F32),
        in_specs=[pl.BlockSpec(memory_space=pl.ANY)] * 2,
        out_specs=pl.BlockSpec(memory_space=pltpu.VMEM),
        scratch_shapes=[
            pltpu.VMEM((CHUNKS, ALL, WIDTH), BF16),
            pltpu.VMEM((6, 6, ALL, 128), F32),
            pltpu.VMEM((6, 3, ALL, 128), F32),
            pltpu.VMEM((ALL, 2 * WIDTH), BF16),
            pltpu.VMEM((7, CHUNKS, WIDTH), F32),
            pltpu.VMEM((6, CHUNKS, WIDTH), F32),
            pltpu.VMEM((3, 32, 128), F32),
            pltpu.VMEM((16, 128), F32),
            pltpu.VMEM((3, 2, 2, 8, 128), F32),
            pltpu.VMEM((12, 8, 128), F32),
            pltpu.VMEM((2, 1, 128), F32),
            pltpu.VMEM((16, 1, 128), F32),
            pltpu.VMEM((8, 1, 128), F32),
            dma((EARLY + 1,)),
            dma,
            dma((EARLY + 1,)),
            dma,
            dma((6,)),
            dma,
            dma((2, CHUNKS)),
            dma((PAIRS,)),
            dma,
            dma((6,)),
            dma,
            dma,
            dma,
            dma,
            dma,
            dma,
        ],
        compiler_params=pltpu.CompilerParams(collective_id=0, has_side_effects=True, vmem_limit_bytes=60 * 2**20),
    )(text_features, vision_features)
    return pl.pallas_call(
        write,
        out_shape=(
            jax.ShapeDtypeStruct((HALF, LA * LB), F32),
            jax.ShapeDtypeStruct((LA, LB), F32),
        ),
        in_specs=[pl.BlockSpec(memory_space=pltpu.VMEM)],
        out_specs=(pl.BlockSpec(memory_space=pltpu.VMEM),) * 2,
    )(raw)


def solution(mesh):
    split = Mesh(mesh.devices.reshape(4, 2, 4, 4), ("row_0", "row_1", "col_0", "col_1"))
    rows = ("row_0", "row_1", "col_0", "col_1")
    placed = (P(None, rows, None), P(None, rows, None))
    return jax.shard_map(local, mesh=split, in_specs=placed, out_specs=(P(rows, None), P()), check_vma=False)
```

```python
import jax
import jax.numpy as jnp
from jax import lax
from jax.experimental import pallas as pl
from jax.experimental.pallas import tpu as pltpu
from jax.sharding import Mesh
from jax.sharding import PartitionSpec as P

STIMULI = 4096
LA, LB = 5, 6
BLOCKS = (
    (0, 1, 0), (0, 0, 2), (3, 0, 0), (2, 0, 0), (1, 3, 0), (1, 1, 1),
    (0, 1, 1), (0, 1, 2), (0, 0, 0), (2, 3, 0), (0, 0, 3), (0, 3, 0),
)
OWN = 8
STRIPS = ((2, 4, 5, 10, 11), (1, 5, 10, 11), (0, 1, 3, 7, 8, 10, 11), (1, 3, 4, 9, 11), (0, 1, 5, 6, 10), (3, 4, 5, 6, 9, 10))
STEPS = ((1, 0, 0), (3, 0, 0), (0, 1, 0), (0, 3, 0), (0, 0, 1), (0, 0, 3))
EDGES = (
    ((8, 0, 2), (8, 2, 1), (8, 10, 5), (8, 11, 3)),
    ((10, 1, 5), (2, 3, 1), (11, 4, 0), (0, 6, 4)),
    ((6, 5, 0), (1, 7, 2), (3, 9, 3)),
)
CHUNKS, WIDTH = 48, 256
PAIRS = CHUNKS // 2
ROWS, HALF = 64, 32
ALL = len(BLOCKS) * ROWS
EARLY, LAG, LATE, PACE = 4, 4, 4, 4
LAST = (3, 10, 17, 19, 21, 23)
F32, BF16 = jnp.float32, jnp.bfloat16
MESH = pl.DeviceIdType.MESH


def kernel(
    text, vision, raw,
    buf, acc, rx, xc, sums, mrx, rs, selfs, pack, rrx, row, ar1, ar2,
    load_sem, swap_send, swap_recv, mean_send, mean_recv, hop_send, hop_recv, last_recv,
    ex_send, ex_recv, rs_send, rs_recv, ar1_send, ar1_recv, ar2_send, ar2_recv,
):
    y, p = lax.axis_index("row_0"), lax.axis_index("row_1")
    z, x = lax.axis_index("col_0"), lax.axis_index("col_1")

    def at(offset, core):
        dx, dy, dz = offset
        return (lax.rem(y + dy, 4), core, lax.rem(z + dz, 4), lax.rem(x + dx, 4))

    def back(step):
        return tuple((4 - v) % 4 for v in step)

    def remote(src, dst, send, recv, device):
        return pltpu.make_async_remote_copy(
            src_ref=src, dst_ref=dst, send_sem=send, recv_sem=recv, device_id=device, device_id_type=MESH
        )

    other = 1 - p
    here = (0, 0, 0)

    def source(c, core):
        if c < 8:
            return text.at[2, :, pl.ds(pl.multiple_of(core * 1536 + c * WIDTH, WIDTH), WIDTH)]
        if c < 22:
            return text.at[core * 3, :, pl.ds((c - 8) * WIDTH, WIDTH)]
        if c < 36:
            return text.at[core * 3 + 1, :, pl.ds((c - 22) * WIDTH, WIDTH)]
        return vision.at[core * 3 + (c - 36) // 4, :, pl.ds((c - 36) % 4 * WIDTH, WIDTH)]

    first = 2 * p
    mine = pl.ds(pl.multiple_of(OWN * ROWS + p * HALF, HALF), HALF)

    def load(c):
        return pltpu.make_async_copy(source(c, p), buf.at[c, mine, :], load_sem.at[min(c, EARLY)])

    def swap(c):
        return remote(source(c, other), buf.at[c, mine, :], swap_send, swap_recv.at[min(c, EARLY)], at(here, other))

    for c in range(CHUNKS):
        if c < 2:
            pl.when(p == 0)(lambda c=c: load(c).start())
        else:
            load(c).start()

    barrier = pltpu.get_barrier_semaphore()
    greeted = [at(step, p) for step in STEPS]
    greeted.append(at(here, other))
    for device in greeted:
        pl.semaphore_signal(barrier, inc=1, device_id=device, device_id_type=MESH)
    pl.semaphore_wait(barrier, len(greeted))

    for c in range(CHUNKS):
        if c < 2:
            pl.when(p == 1)(lambda c=c: swap(c).start())
        else:
            swap(c).start()

    @pl.loop(0, 36)
    def _(i):
        acc[i // 6, i % 6] = jnp.zeros((ALL, 128), F32)

    rs[...] = jnp.zeros_like(rs)
    selfs[...] = jnp.zeros_like(selfs)

    def hop(edge, c):
        held, becomes, step = edge
        return remote(
            buf.at[c, pl.ds(held * ROWS, ROWS), :],
            buf.at[c, pl.ds(becomes * ROWS, ROWS), :],
            hop_send,
            last_recv.at[c // 2] if kind[becomes] == 2 else hop_recv.at[kind[becomes], c],
            at(back(STEPS[step]), p),
        )

    inner = [sorted({e[0] for e in EDGES[d]}) for d in range(3)]
    kind = {e[1]: next((d - 1 for d in (1, 2) if e[1] in inner[d]), 2) for d in EDGES for e in d}

    def arrived(which, c):
        part = buf.at[c, pl.ds(0, ROWS * sum(k == which for k in kind.values())), :]
        pltpu.make_async_copy(part, part, hop_recv.at[which, c]).wait()

    def arrived_pair(k):
        part = buf.at[pl.ds(2 * k, 2), pl.ds(0, ROWS * sum(k == 2 for k in kind.values())), :]
        pltpu.make_async_copy(part, part, last_recv.at[k]).wait()

    def send_own(c):
        for edge in EDGES[0]:
            hop(edge, c).start()

    where = (x, y, z)

    def mean_copy(n):
        axis, second = n // 2, n % 2
        place = list(where)
        place[axis] = 3 - where[axis] if second else where[axis] + 1 - 2 * lax.rem(where[axis], 2)
        device = (place[1], p, place[2], place[0])
        return remote(sums.at[n], mrx.at[n], mean_send, mean_recv.at[n], device)

    def exchange(layer):
        for core in (0, 1):

            @pl.when(p == core)
            def _():
                for i in range(3):
                    q = (1 - core) * 3 + i
                    for block in STRIPS[q]:
                        strip = pl.ds(block * ROWS, ROWS)
                        remote(
                            acc.at[layer, q, strip],
                            rx.at[layer, i, strip],
                            ex_send,
                            ex_recv.at[layer],
                            at(here, other),
                        ).start()

    def exchanged(sem):
        part = acc.at[0, pl.ds(0, 2), pl.ds(0, 8 * ROWS)]
        pltpu.make_async_copy(part, part, sem).wait()

    def products(core, k):
        texts = (0, 1, 2, 3, 4) if core == 0 else (3, 4, 2, 0, 1)
        for i in range(3):
            q = core * 3 + i
            n_text = LA if k == 0 else 0

            def body(r, sums_):
                s = list(sums_)
                for block in STRIPS[q]:
                    at_ = pl.ds(pl.multiple_of(block * ROWS + r * 8, 8), 8)
                    t = (
                        acc[1, q, at_, :],
                        acc[2, q, at_, :],
                        acc[0, q, at_, :] + rx[0, i, at_, :],
                        rx[1, i, at_, :],
                        rx[2, i, at_, :],
                    )
                    v = (acc[3 + k, q, at_, :], rx[3 + k, i, at_, :])
                    for a in range(LA):
                        for b in range(2):
                            s[2 * a + b] += t[a] * v[b]
                    for b in range(2):
                        s[10 + b] += v[b] * v[b]
                    for a in range(n_text):
                        s[12 + a] += t[a] * t[a]
                return tuple(s)

            zero = jnp.zeros((8, 128), F32)
            s = lax.fori_loop(0, 8, body, (zero,) * (12 + n_text))
            visions = (core * 3 + k, (1 - core) * 3 + k)
            for a in range(LA):
                for b in range(2):
                    n = texts[a] * LB + visions[b]
                    rs[i, n : n + 1, :] = jnp.sum(s[2 * a + b], axis=0, keepdims=True)
            for b in range(2):
                n = 8 + visions[b]
                selfs[n : n + 1, :] += jnp.sum(s[10 + b], axis=0, keepdims=True)
            for a in range(n_text):
                n = texts[a]
                selfs[n : n + 1, :] += jnp.sum(s[12 + a], axis=0, keepdims=True)

    def compute(k):
        arrived_pair(k)
        for h in range(2):
            mean = sums[6, pl.ds(2 * k + h, 1), :] * (1.0 / STIMULI)
            xc[:, h * WIDTH : (h + 1) * WIDTH] = (buf[2 * k + h].astype(F32) - mean).astype(BF16)
        layer = jnp.where(k < 4, 0, jnp.where(k < 11, 1, jnp.where(k < 18, 2, 3 + (k - 18) // 2)))
        for g in range(3):
            blocks = sorted({*STRIPS[2 * g], *STRIPS[2 * g + 1]})
            tile = lax.dot_general(
                jnp.concatenate([xc[b * ROWS : (b + 1) * ROWS, :] for b in blocks], axis=0),
                xc[g * 256 : (g + 1) * 256, :],
                (((1,), (1,)), ((), ())),
                preferred_element_type=F32,
            )
            for n, b in enumerate(blocks):
                strip = slice(b * ROWS, (b + 1) * ROWS)
                for h in range(2):
                    if b in STRIPS[2 * g + h]:
                        acc[layer, 2 * g + h, strip] += tile[n * ROWS : (n + 1) * ROWS, h * 128 : (h + 1) * 128]
        for layer, last in enumerate(LAST):
            pl.when(k == last)(lambda layer=layer: exchange(layer))
        for n in (0, 1):

            @pl.when(k == LAST[3 + n] + 1)
            def _():
                for layer in (0, 1, 2, 3) if n == 0 else (4,):
                    exchanged(ex_recv.at[layer])
                for core in (0, 1):
                    pl.when(p == core)(lambda core=core: products(core, n))


    def computed(u):
        ready = jnp.minimum((u - LAG - LATE + 1) // 2, u - (6 * PACE - 1))
        return jnp.minimum(jnp.maximum(ready, p), PAIRS)

    def send_half(c, core):
        for held, becomes, step in EDGES[0]:
            rows = [pl.ds(pl.multiple_of(b * ROWS + core * HALF, HALF), HALF) for b in (held, becomes)]
            remote(
                buf.at[c, rows[0], :],
                buf.at[c, rows[1], :],
                hop_send,
                last_recv.at[c // 2] if kind[becomes] == 2 else hop_recv.at[kind[becomes], c],
                at(back(STEPS[step]), p),
            ).start()

    @pl.loop(first, EARLY)
    def _(c):
        part = buf.at[c, mine, :]
        pltpu.make_async_copy(part, part, load_sem.at[c]).wait()
        send_half(c, p)

    @pl.loop(first, EARLY)
    def _(c):
        part = buf.at[c, mine, :]
        pltpu.make_async_copy(part, part, swap_recv.at[c]).wait()
        send_half(c, other)

    rest = buf.at[pl.ds(EARLY, CHUNKS - EARLY), mine, :]
    pltpu.make_async_copy(rest, rest, load_sem.at[EARLY]).wait()
    pltpu.make_async_copy(rest, rest, swap_recv.at[EARLY]).wait()

    for c in range(CHUNKS):
        total = jnp.sum(buf[c, OWN * ROWS : (OWN + 1) * ROWS, :].astype(F32), axis=0, keepdims=True)
        sums[0, c : c + 1, :] = jnp.where(p == 1, 0.0, total) if c < 2 else total

    mean_copy(0).start()

    @pl.loop(0, CHUNKS + LAG + LATE)
    def _(u):
        for n in range(1, 6):
            pl.when(u == PACE * n)(lambda n=n: mean_copy(n).start())

        @pl.when(u + EARLY < CHUNKS)
        def _():
            send_own(u + EARLY)

        for depth in (2, 1):
            c = u - (depth - 1) * LAG

            @pl.when((c >= first) & (c < CHUNKS))
            def _():
                arrived(depth - 1, c)
                for edge in EDGES[depth]:
                    hop(edge, c).start()

        for n in range(6):

            @pl.when(u == PACE * n + PACE - 1)
            def _():
                mean_copy(n).wait_recv()
                sums[n + 1] = sums[n] + mrx[n]

        @pl.loop(computed(u - 1), computed(u))
        def _(k):
            compute(k)

    exchanged(ex_recv.at[5])

    lanes8 = lax.broadcasted_iota(jnp.int32, (8, 128), 1)

    def deliver(core):
        for i in range(3):
            q = core * 3 + i
            for j in (2 * q, 2 * q + 1):
                for to in (0, 1):
                    first = j % 2 * ROWS + to * HALF
                    tile = jnp.zeros((8, 128), F32)
                    for g in range(4):
                        turned = rs[i, 8 * g : 8 * g + 8, :]
                        if (g * HALF - first) % 128:
                            turned = pltpu.roll(turned, (g * HALF - first) % 128, 1)
                        tile = jnp.where(lanes8 // HALF == g, turned, tile)
                    if j == OWN and to == core:
                        rrx[j] = tile
                    else:
                        pack[i, j % 2, to] = tile
            for j in (2 * q, 2 * q + 1):
                for to in (0, 1):
                    if not (j == OWN and to == core):
                        share(i, j, to).start()

    def share(i, j, to):
        return remote(pack.at[i, j % 2, to], rrx.at[j], rs_send, rs_recv, at(BLOCKS[j], to))

    for core in (0, 1):

        @pl.when(p == core)
        def _():
            products(core, 2)

    cross = rs[0] + rs[1] + rs[2]
    parts = jnp.concatenate([cross, selfs[...]], axis=0)
    parts = jnp.sum(parts, axis=1, keepdims=True)
    lane = lax.broadcasted_iota(jnp.int32, (48, 128), 1)
    sub = lax.broadcasted_iota(jnp.int32, (48, 128), 0)
    row[0] = jnp.sum(jnp.where(lane == sub, parts, 0.0), axis=0, keepdims=True)

    plane = [(dx, dy) for dx in range(4) for dy in range(4) if dx or dy]
    me1 = x * 4 + y

    def over_plane(n):
        dx, dy = plane[n]
        return remote(row.at[0], ar1.at[me1], ar1_send, ar1_recv, at((dx, dy, 0), p))

    for n in range(15):
        over_plane(n).start()
    for core in (0, 1):
        pl.when(p == core)(lambda core=core: deliver(core))
    ar1[me1] = row[0]
    others1 = ar1.at[pl.ds(0, 15)]
    pltpu.make_async_copy(others1, others1, ar1_recv).wait()
    row[1] = jnp.sum(ar1[...], axis=0)

    column = [(dz, dc) for dz in range(4) for dc in range(2) if dz or dc]
    me2 = z * 2 + p

    def over_column(n):
        dz, dc = column[n]
        return remote(
            row.at[1], ar2.at[me2], ar2_send, ar2_recv, at((0, 0, dz), other if dc else p)
        )

    for n in range(7):
        over_column(n).start()
    ar2[me2] = row[1]
    others2 = ar2.at[pl.ds(0, 7)]
    pltpu.make_async_copy(others2, others2, ar2_recv).wait()
    total = jnp.sum(ar2[...], axis=0)

    def pick(index, n):
        lanes = lax.broadcasted_iota(jnp.int32, (n, 128), 1)
        return jnp.sum(jnp.where(lanes == index, total, 0.0), axis=1, keepdims=True)

    pair = lax.broadcasted_iota(jnp.int32, (32, 1), 0)
    of_text, of_vision = pair // LB, lax.rem(pair, LB)
    scale = 1.0 / jnp.sqrt(pick(32 + jnp.minimum(of_text, LA - 1), 32) * pick(40 + of_vision, 32))
    def tiles(core, sem):
        part = rrx.at[pl.ds(0, len(BLOCKS) - (core == OWN // 6))]
        pltpu.make_async_copy(part, part, sem).wait()

    for core in (0, 1):
        pl.when(p == core)(lambda core=core: tiles(core, rs_recv))
    packed = ((rrx[0] + rrx[1]) + (rrx[2] + rrx[3])) + ((rrx[4] + rrx[5]) + (rrx[6] + rrx[7]))
    packed += (rrx[8] + rrx[9]) + (rrx[10] + rrx[11])
    share_sum = jnp.concatenate([packed] + [pltpu.roll(packed, 128 - g * HALF, 1) for g in (1, 2, 3)], axis=0)
    raw[0:32] = share_sum * (scale * STIMULI)

    a_sub = lax.broadcasted_iota(jnp.int32, (8, 1), 0)
    spread = jnp.broadcast_to(total, (8, 128))
    crosses = spread
    for a in range(1, LA):
        crosses = jnp.where(a_sub == a, pltpu.roll(spread, 128 - a * LB, 1), crosses)
    text_self = pick(32 + jnp.minimum(a_sub, LA - 1), 8)
    vision_self = pltpu.roll(spread, 128 - 40, 1)
    raw[32:37, :LB] = crosses[:LA, :LB] * (1.0 / jnp.sqrt(text_self[:LA] * vision_self[:LA, :LB]))

    def drain(core):
        crossed = buf.at[pl.ds(0, CHUNKS - 2 * (1 - core)), pl.ds(0, HALF), :]
        hopped = buf.at[pl.ds(0, CHUNKS - 2 * core), pl.ds(0, ALL - ROWS), :]
        pltpu.make_async_copy(crossed, crossed, swap_send).wait()
        pltpu.make_async_copy(hopped, hopped, hop_send).wait()
        tiles(core, rs_send)

    for core in (0, 1):
        pl.when(p == core)(lambda core=core: drain(core))
    means = sums.at[pl.ds(0, 6)]
    pltpu.make_async_copy(means, means, mean_send).wait()
    strips = acc.at[pl.ds(0, 6), pl.ds(0, 2), pl.ds(0, 8 * ROWS)]
    pltpu.make_async_copy(strips, strips, ex_send).wait()
    pltpu.make_async_copy(others1, others1, ar1_send).wait()
    pltpu.make_async_copy(others2, others2, ar2_send).wait()


def write(raw, terms, cka):
    terms[...] = jnp.transpose(raw[0:32])[:HALF, : LA * LB]
    cka[...] = raw[32:37, :LB]


def local(text_features, vision_features):
    dma = pltpu.SemaphoreType.DMA
    raw = pl.pallas_call(
        kernel,
        out_shape=jax.ShapeDtypeStruct((40, 128), F32),
        in_specs=[pl.BlockSpec(memory_space=pl.ANY)] * 2,
        out_specs=pl.BlockSpec(memory_space=pltpu.VMEM),
        scratch_shapes=[
            pltpu.VMEM((CHUNKS, ALL, WIDTH), BF16),
            pltpu.VMEM((6, 6, ALL, 128), F32),
            pltpu.VMEM((6, 3, ALL, 128), F32),
            pltpu.VMEM((ALL, 2 * WIDTH), BF16),
            pltpu.VMEM((7, CHUNKS, WIDTH), F32),
            pltpu.VMEM((6, CHUNKS, WIDTH), F32),
            pltpu.VMEM((3, 32, 128), F32),
            pltpu.VMEM((16, 128), F32),
            pltpu.VMEM((3, 2, 2, 8, 128), F32),
            pltpu.VMEM((12, 8, 128), F32),
            pltpu.VMEM((2, 1, 128), F32),
            pltpu.VMEM((16, 1, 128), F32),
            pltpu.VMEM((8, 1, 128), F32),
            dma((EARLY + 1,)),
            dma,
            dma((EARLY + 1,)),
            dma,
            dma((6,)),
            dma,
            dma((2, CHUNKS)),
            dma((PAIRS,)),
            dma,
            dma((6,)),
            dma,
            dma,
            dma,
            dma,
            dma,
            dma,
        ],
        compiler_params=pltpu.CompilerParams(collective_id=0, has_side_effects=True, vmem_limit_bytes=60 * 2**20),
    )(text_features, vision_features)
    return pl.pallas_call(
        write,
        out_shape=(
            jax.ShapeDtypeStruct((HALF, LA * LB), F32),
            jax.ShapeDtypeStruct((LA, LB), F32),
        ),
        in_specs=[pl.BlockSpec(memory_space=pltpu.VMEM)],
        out_specs=(pl.BlockSpec(memory_space=pltpu.VMEM),) * 2,
    )(raw)


def solution(mesh):
    split = Mesh(mesh.devices.reshape(4, 2, 4, 4), ("row_0", "row_1", "col_0", "col_1"))
    rows = ("row_0", "row_1", "col_0", "col_1")
    placed = (P(None, rows, None), P(None, rows, None))
    return jax.shard_map(local, mesh=split, in_specs=placed, out_specs=(P(rows, None), P()), check_vma=False)
```
